32 devices in a mesh: fsdp: 4 (over y, x), seq: 8 (over z, core).
Axes of the slice: x: 2, y: 2, z: 4, core: 2. Of those that a mesh axis runs over, the one named last changes fastest.
Arguments:
- image_input: bfloat16 [4, 1024, 1536], P('fsdp', 'seq'), may hold values from -6 to 6
- text_input: bfloat16 [4, 128, 1536], P('fsdp'), may hold values from -6 to 6
- w_qkv: bfloat16 [1536, 3, 2048], P('fsdp'), may hold values from -0.15625 to 0.15625
- query_gain: float32 [128], replicated, may hold values from 1.2 to 2.4
- key_gain: float32 [128], replicated, may hold values from 1.2 to 2.4
- image_cotangent: bfloat16 [4, 1024, 2048], P('fsdp', 'seq'), may hold values from -6 to 6
- text_cotangent: bfloat16 [4, 128, 2048], P('fsdp'), may hold values from -6 to 6
Outputs:
- image_grad: bfloat16 [4, 1024, 1536], P('fsdp', 'seq')
- text_grad: bfloat16 [4, 128, 1536], P('fsdp')
- weight_grad: float32 [1536, 3, 2048], P('fsdp', None, 'seq')
- gain_grad: float32 [2, 128], replicated
The draws below stay inside these ranges and needn't reach their ends.
All inputs are finite; a program needn't handle non-finite values.
Results may differ from the reference program's by a relative error of at most 0.018.
The reference program's roundings to bfloat16 on the way count: a program that leaves them out, or rounds other values in their place, can miss the bound.
Values may be sent and summed in bfloat16 or wider, within the bound.
A program may use at most 192 MiB of HBM per device.

```python
import math
import jax
import jax.numpy as jnp
from jax import lax

D = 1536
HEADS = 16
HEAD = 128
TXT = 128
IMG_DEV = 128
B_DEV = 1
BATCH = 4
IMG = 1024
N_FSDP = 4
N_SEQ = 8


def steps_of(own_key, dims, cuts, smallest, high):
    factor_of, own = 1.0, jax.random.fold_in(own_key, 6)
    for dim, shards_of in cuts:
        steps = jnp.exp(jax.random.uniform(jax.random.fold_in(own, dim), (shards_of,), jnp.float32, smallest / len(cuts), high / len(cuts)))
        factor_of = factor_of * jnp.repeat(steps, dims[dim] // shards_of).reshape([-1 if axis == dim else 1 for axis in range(len(dims))])
    return factor_of


def gaussian(rng, shape, scale, reach, cuts=(), kind=jnp.bfloat16):
    result = jax.random.normal(rng, shape, jnp.float32) * scale
    if len(cuts) > 0:
        result = steps_of(rng, shape, cuts, -0.22, 0.18) * result
    return jnp.clip(result, min=-reach, max=reach).astype(kind)


def setup_inputs(seed: int = 0) -> dict:
    key_list = jax.random.split(jax.random.key(seed), 8)
    image_input = gaussian(key_list[0], (BATCH, IMG, D), 1.0, 6.0, ((0, 4), (1, 8)))
    text_input = gaussian(key_list[1], (BATCH, TXT, D), 1.0, 6.0, ((0, 4),))
    w_qkv = gaussian(key_list[2], (D, 3, HEADS * HEAD), D ** -0.5, 0.15625, ((0, 4),))
    query_gain = jnp.clip(jnp.exp(jax.random.uniform(key_list[3], (HEAD,), jnp.float32, math.log(1.2), math.log(2.4))), 1.2, 2.4)
    key_gain = jnp.clip(jnp.exp(jax.random.uniform(key_list[4], (HEAD,), jnp.float32, math.log(1.2), math.log(2.4))), 1.2, 2.4)
    image_cotangent = gaussian(key_list[5], (BATCH, IMG, HEADS * HEAD), 1.0, 6.0, ((0, 4), (1, 8)))
    text_cotangent = gaussian(key_list[6], (BATCH, TXT, HEADS * HEAD), 1.0, 6.0, ((0, 4),))
    return dict(image_input=image_input, text_input=text_input, w_qkv=w_qkv, query_gain=query_gain, key_gain=key_gain, image_cotangent=image_cotangent, text_cotangent=text_cotangent)


epsilon = 1e-06
query_parts = 4

def rms_forward(values, gain):
    floated = values.astype(jnp.float32)
    inverse = lax.rsqrt(lax.optimization_barrier(jnp.mean(floated * floated, axis=-1, keepdims=True)) + epsilon)
    return (floated, inverse, (floated * inverse * gain).astype(jnp.bfloat16))

def rms_backward(floated, inverse, gain, incoming):
    weighted = incoming * gain
    inner_mean = lax.optimization_barrier(jnp.mean(weighted * floated, axis=-1, keepdims=True))
    grad_input = inverse * weighted - floated * inverse * inverse * inverse * inner_mean
    grad_gain = lax.optimization_barrier(jnp.sum(incoming * floated * inverse, axis=0))
    return (grad_input, grad_gain)

def head_backward(query_rows, key_rows, value_rows, incoming, query_gain, key_gain):
    query_float, query_inverse, query_normed = rms_forward(query_rows, query_gain)
    key_float, key_inverse, key_normed = rms_forward(key_rows, key_gain)
    length = query_rows.shape[0]
    width = query_rows.shape[1]
    block_rows = length // query_parts
    factor = 1.0 / math.sqrt(width)
    query_blocks = query_normed.reshape(query_parts, block_rows, width)
    incoming_blocks = incoming.reshape(query_parts, block_rows, width)

    def visit(carried, pieces):
        key_total, value_total = carried
        query_piece, incoming_piece = pieces
        scores = jnp.dot(query_piece, key_normed.T, preferred_element_type=jnp.float32) * factor
        attention = jax.nn.softmax(scores, axis=-1)
        attention_grad = jnp.dot(incoming_piece, value_rows.T, preferred_element_type=jnp.float32)
        row_dot = lax.optimization_barrier(jnp.sum(attention * attention_grad, axis=-1, keepdims=True))
        score_grad = (attention * (attention_grad - row_dot)).astype(jnp.bfloat16)
        value_total = value_total + jnp.dot(attention.astype(jnp.bfloat16).T, incoming_piece, preferred_element_type=jnp.float32)
        key_total = key_total + jnp.dot(score_grad.T, query_piece, preferred_element_type=jnp.float32) * factor
        query_grad = jnp.dot(score_grad, key_normed, preferred_element_type=jnp.float32) * factor
        return ((key_total, value_total), query_grad)
    zeros_init = jnp.zeros((length, width), jnp.float32)
    (key_total, value_total), query_pieces = lax.scan(visit, (zeros_init, zeros_init), (query_blocks, incoming_blocks))
    query_grad = query_pieces.reshape(length, width)
    query_input_grad, query_gain_grad = rms_backward(query_float, query_inverse, query_gain, query_grad)
    key_input_grad, key_gain_grad = rms_backward(key_float, key_inverse, key_gain, key_total)
    stacked = jnp.stack([query_input_grad, key_input_grad, value_total], axis=1).astype(jnp.bfloat16)
    return (stacked, jnp.stack([query_gain_grad, key_gain_grad], axis=0))

def reference(image_input, text_input, w_qkv, query_gain, key_gain, image_cotangent, text_cotangent):
    tokens = jnp.concatenate([text_input, image_input], axis=1)
    upstream = jnp.concatenate([text_cotangent, image_cotangent], axis=1)
    weights = w_qkv.astype(jnp.float32)
    triple = jnp.einsum('btd,dch->btch', tokens.astype(jnp.float32), weights).astype(jnp.bfloat16)
    batch_count = triple.shape[0]
    length = triple.shape[1]
    by_heads = triple.reshape(batch_count, length, 3, HEADS, HEAD).transpose(0, 3, 1, 2, 4).reshape(batch_count * HEADS, length, 3, HEAD)
    incoming_heads = upstream.reshape(batch_count, length, HEADS, HEAD).transpose(0, 2, 1, 3).reshape(batch_count * HEADS, length, HEAD)

    def one_head(pair):
        inputs, incoming = pair
        return head_backward(inputs[:, 0], inputs[:, 1], inputs[:, 2], incoming, query_gain, key_gain)
    all_grads, gain_rows = lax.map(one_head, (by_heads, incoming_heads))
    triple_grad = all_grads.reshape(batch_count, HEADS, length, 3, HEAD).transpose(0, 2, 3, 1, 4).reshape(batch_count, length, 3, HEADS * HEAD)
    gain_grad = lax.optimization_barrier(jnp.sum(gain_rows, axis=0))
    full_grad = jnp.einsum('btch,dch->btd', triple_grad.astype(jnp.float32), weights).astype(jnp.bfloat16)
    text_grad = full_grad[:, :TXT]
    image_grad = full_grad[:, TXT:]
    head_group = jnp.arange(HEADS * HEAD, dtype=jnp.int32) // (HEAD * (HEADS // N_SEQ))
    zero_index = jnp.zeros((), jnp.int32)

    def over_groups(group_index, running):
        first_row = (group_index * B_DEV).astype(jnp.int32)
        text_block = lax.dynamic_slice_in_dim(text_input, first_row, B_DEV, 0).astype(jnp.float32)
        text_block_grad = lax.dynamic_slice_in_dim(triple_grad[:, :TXT], first_row, B_DEV, 0).astype(jnp.float32)
        text_part = jnp.einsum('btd,btch->dch', text_block, text_block_grad)

        def over_members(member_index, running_inner):
            image_start = (member_index * IMG_DEV).astype(jnp.int32)
            image_block = lax.dynamic_slice(image_input, (first_row, image_start, zero_index), (B_DEV, IMG_DEV, D)).astype(jnp.float32)
            block_grads = lax.dynamic_slice(triple_grad, (first_row, image_start + TXT, zero_index, zero_index), (B_DEV, IMG_DEV, 3, HEADS * HEAD)).astype(jnp.float32)
            column_mask = (head_group == member_index).astype(jnp.float32)
            partial_value = jnp.einsum('btd,btch->dch', image_block, block_grads) + text_part * column_mask
            rounded = lax.optimization_barrier(partial_value.astype(jnp.bfloat16))
            return running_inner + rounded.astype(jnp.float32)
        return lax.fori_loop(0, N_SEQ, over_members, running)
    weight_grad = lax.fori_loop(0, N_FSDP, over_groups, jnp.zeros((D, 3, HEADS * HEAD), jnp.float32))
    return (image_grad, text_grad, weight_grad, gain_grad)
```

```python
import functools
import math

import jax
import jax.numpy as jnp
from jax import lax
from jax.experimental import pallas as pl
from jax.experimental.pallas import tpu as pltpu
from jax.sharding import PartitionSpec as P

EPSILON = 1e-06
MESH = pl.DeviceIdType.MESH
F32 = jnp.float32
BF16 = jnp.bfloat16
NT = (((1,), (1,)), ((), ()))
CHUNKS = 2


def kernel(
    nf, ns, image_ref, text_ref, weight_ref, up_ref, text_up_ref, qg_ref, kg_ref,
    image_out, text_out, weight_out, gain_out,
    tokens, weights, ups, triple, grads, qn_s, kn_s, knt_s, dq_s, dk_s, dv_s,
    sib_send, sib_recv, mine, line_send, line_recv, w_send, w_recv, gain_all, gain_rows,
    text_share, tokens_t,
    x_send, x_recv, u_send, u_recv, wg_send, wg_recv, sb_send, sb_recv,
    zs_send, zs_recv, ws_send, ws_recv, g_send, g_recv, h_send, h_recv, t_send, t_recv, l_sem,
):
    f = lax.axis_index("fsdp")
    s = lax.axis_index("seq")
    nz = ns // 2
    z = lax.div(s, 2)
    core = lax.rem(s, 2)
    other = 1 - core
    sib = z * 2 + other
    rows = image_ref.shape[0]
    text_rows = text_ref.shape[0]
    parts, w_rows, all_width = weight_ref.shape
    own_width = all_width // ns
    head = qg_ref.shape[1]
    heads = own_width // head
    length = tokens.shape[0]
    piece = text_rows // ns
    chunk = rows // CHUNKS
    half = w_rows // 2
    pending = []

    def remote(src, dst, send, recv, target):
        return pltpu.make_async_remote_copy(
            src_ref=src, dst_ref=dst, send_sem=send, recv_sem=recv,
            device_id=target, device_id_type=MESH,
        )

    def launch(copy, where=None):
        if where is None:
            copy.start()
        else:
            pl.when(where)(copy.start)
        pending.append((where, copy))

    def rank(at, who):
        away = jnp.abs(who - at)
        nearer = jnp.minimum(away - 1, at) + jnp.minimum(away - 1, nz - 1 - at)
        second = jnp.where((who > at) & (at >= away), 1, 0)
        return jnp.where(away == 0, 0, 1 + nearer + second)

    def place(at, who, which):
        return pl.multiple_of(text_rows + (rank(at, who) * 2 + which) * rows, rows)

    def w_at(index):
        return pl.ds(pl.multiple_of(index * w_rows, w_rows), w_rows)

    def u_at(index):
        return pl.ds(pl.multiple_of(index * own_width, own_width), own_width)

    own_at = pl.ds(place(z, z, core), rows)
    locals_ = [
        pltpu.make_async_copy(
            weight_ref.at[c, :, u_at(s)],
            weights.at[w_at(f), pl.ds(c * own_width, own_width)],
            l_sem.at[4 + c],
        )
        for c in range(parts)
    ] + [
        pltpu.make_async_copy(image_ref, tokens.at[own_at], l_sem.at[0]),
        pltpu.make_async_copy(text_ref, tokens.at[pl.ds(0, text_rows)], l_sem.at[1]),
        pltpu.make_async_copy(up_ref.at[:, u_at(s)], ups.at[own_at], l_sem.at[2]),
        pltpu.make_async_copy(
            text_up_ref.at[:, u_at(s)], ups.at[pl.ds(0, text_rows)], l_sem.at[3]
        ),
    ]
    for copy in locals_:
        copy.start()

    barrier = pltpu.get_barrier_semaphore()
    for k in range(1, nf):
        pl.semaphore_signal(
            barrier, inc=1, device_id=(lax.rem(f + k, nf), s), device_id_type=MESH
        )
    for k in range(1, ns):
        pl.semaphore_signal(
            barrier, inc=1, device_id=(f, lax.rem(s + k, ns)), device_id_type=MESH
        )
    pl.semaphore_wait(barrier, nf + ns - 2)

    up_ok = z < nz - 1
    down_ok = z > 0

    def x_copy(source, which, ch, to_z, to_core, own=False):
        src = (
            image_ref.at[pl.ds(ch * chunk, chunk)]
            if own
            else tokens.at[pl.ds(place(z, source, which) + ch * chunk, chunk)]
        )
        return remote(
            src,
            tokens.at[pl.ds(place(to_z, source, which) + ch * chunk, chunk)],
            x_send.at[len(x_count)],
            x_recv.at[rank(to_z, source) * 2 + which, ch],
            (f, to_z * 2 + to_core),
        )

    x_count = []

    def x_launch(*args, where=None, **kw):
        copy = x_copy(*args, **kw)
        x_count.append(0)
        launch(copy, where)

    def x_wait(source, which, ch):
        remote(
            image_ref.at[pl.ds(0, chunk)],
            tokens.at[pl.ds(place(z, source, which) + ch * chunk, chunk)],
            x_send.at[0], x_recv.at[rank(z, source) * 2 + which, ch], (f, s),
        ).wait_recv()

    for ch in range(CHUNKS):
        x_launch(z, core, ch, z + 1, core, own=True, where=up_ok)
        x_launch(z, core, ch, z - 1, core, own=True, where=down_ok)
        x_launch(z, core, ch, z, other, own=True)

    fast = lax.rem(f, 2)
    slow = lax.div(f, 2)
    na = nf // 2
    partner = slow * 2 + 1 - fast
    around = [lax.rem(slow + j, na) for j in range(1, na)]
    peers = [a * 2 + fast for a in around]
    corners = [a * 2 + 1 - fast for a in around]

    def w_half(source, hf):
        return weights.at[pl.ds(pl.multiple_of(source * w_rows + hf * half, half), half)]

    w_count = []

    def w_launch(source, hf, target):
        copy = remote(
            w_half(source, hf), w_half(source, hf), wg_send.at[len(w_count)],
            wg_recv.at[source, hf], (target, s),
        )
        w_count.append(0)
        launch(copy)

    def w_wait(source, hf):
        remote(
            w_half(f, hf), w_half(source, hf), wg_send.at[0], wg_recv.at[source, hf], (f, s)
        ).wait_recv()

    for copy in locals_[:parts]:
        copy.wait()
    w_launch(f, 0, partner)
    for q in peers:
        w_launch(f, 1, q)
    w_launch(f, 1, partner)
    for q in peers:
        w_launch(f, 0, q)
    for copy in locals_[parts:]:
        copy.wait()

    def relay_weights():
        w_wait(partner, 0)
        for q in peers:
            w_launch(partner, 0, q)
        for q in peers:
            w_wait(q, 1)
            w_launch(q, 1, partner)

    def finish_weights():
        w_wait(partner, 1)
        for q in peers:
            w_wait(q, 0)
        for q in corners:
            w_wait(q, 0)
            w_wait(q, 1)

    u_count = []

    def u_launch(to_z, to_core, h, where=None):
        column = (to_z * 2 + to_core) * own_width + h * head
        copy = remote(
            up_ref.at[:, pl.ds(pl.multiple_of(column, head), head)],
            ups.at[pl.ds(place(to_z, z, core), rows), pl.ds(h * head, head)],
            u_send.at[len(u_count)],
            u_recv.at[h, rank(to_z, z) * 2 + core],
            (f, to_z * 2 + to_core),
        )
        u_count.append(0)
        launch(copy, where)

    def send_upstream():
        for h in range(heads):
            u_launch(z, other, h)
            for d in range(1, nz):
                for which in (core, other):
                    u_launch(z + d, which, h, where=z + d < nz)
                    u_launch(z - d, which, h, where=z - d >= 0)

    def transpose(start, count):
        at = pl.ds(start, count)
        tokens_t[:, at] = tokens[at, :].T

    def project(start, count):
        at = pl.ds(start, count)
        triple[at, :] = jnp.dot(
            tokens[at, :], weights[...], preferred_element_type=F32
        ).astype(BF16)

    pair = 2 * rows
    first = text_rows + pair
    relayed = False
    for d in range(1, nz):
        sides = (
            (z - d, z - d >= 0, z + 1, up_ok),
            (z + d, z + d < nz, z - 1, down_ok),
        )
        if d == nz - 1:
            if not relayed:
                relay_weights()
                relayed = True
            for ch in range(CHUNKS):
                x_wait(z, other, ch)
            transpose(0, first)
            for k in range(1, nz - 1):
                transpose(first + (k - 1) * pair, pair)
            finish_weights()
            project(0, first)
            for k in range(1, nz - 1):
                project(first + (k - 1) * pair, pair)
        for ch in range(CHUNKS):
            for source, exists, onward, onward_ok in sides:
                pl.when(exists)(functools.partial(x_wait, source, core, ch))
                x_launch(source, core, ch, onward, core, where=exists & onward_ok)
                x_launch(source, core, ch, z, other, where=exists)
            if not relayed:
                relay_weights()
                relayed = True
        for ch in range(CHUNKS):
            for source, exists, onward, onward_ok in sides:
                pl.when(exists)(functools.partial(x_wait, source, other, ch))
        if d == max(1, nz - 2):
            send_upstream()
    last = first + (nz - 2) * pair
    transpose(last, pair)
    project(last, pair)

    factor = 1.0 / math.sqrt(head)
    query_gain = qg_ref[...]
    key_gain = kg_ref[...]
    block = max(b for b in range(128, 385, 128) if length % b == 0)
    per_block = block // rows
    text_pieces = text_rows // rows

    def columns(c, h):
        return pl.ds(c * own_width + h * head, head)

    def inverse_of(values):
        return lax.rsqrt(jnp.mean(values * values, axis=-1, keepdims=True) + EPSILON)

    def rms_backward(values, gain, incoming):
        inverse = inverse_of(values)
        weighted = incoming * gain
        inner = jnp.mean(weighted * values, axis=-1, keepdims=True)
        grad = inverse * weighted - values * (inverse * inverse * inverse * inner)
        return grad, jnp.sum(incoming * values * inverse, axis=0, keepdims=True)

    def u_wait(h, j):
        at = pl.ds(pl.multiple_of(text_rows + j * rows, rows), rows)
        remote(
            up_ref.at[:, pl.ds(0, head)],
            ups.at[at, pl.ds(h * head, head)],
            u_send.at[0], u_recv.at[h, j], (f, s),
        ).wait_recv()

    gain_q = jnp.zeros((1, head), F32)
    gain_k = jnp.zeros((1, head), F32)
    for h in range(heads):
        qf = triple[:, columns(0, h)].astype(F32)
        qn_s[...] = (qf * inverse_of(qf) * query_gain).astype(BF16)
        kf = triple[:, columns(1, h)].astype(F32)
        kn = (kf * inverse_of(kf) * key_gain).astype(BF16)
        kn_s[...] = kn
        knt_s[...] = kn.astype(F32).T.astype(BF16)
        dk_s[...] = jnp.zeros_like(dk_s)
        dv_s[...] = jnp.zeros_like(dv_s)

        def visit(i, carry, h=h):
            for jj in range(per_block):
                j = i * per_block + jj - text_pieces
                pl.when((j >= 0) & (j != core))(functools.partial(u_wait, h, j))
            at = pl.ds(pl.multiple_of(i * block, block), block)
            queries = qn_s[at, :]
            upstream = ups[at, pl.ds(h * head, head)]
            scores = lax.dot_general(kn_s[...], queries, NT, preferred_element_type=F32)
            p = jnp.exp(scores * factor)
            p = p * (1.0 / jnp.sum(p, axis=0, keepdims=True))
            dp = lax.dot_general(
                triple[:, columns(2, h)], upstream, NT, preferred_element_type=F32
            )
            dot = jnp.sum(p * dp, axis=0, keepdims=True)
            ds = (p * (dp - dot)).astype(BF16)
            dv_s[...] += jnp.dot(p.astype(BF16), upstream, preferred_element_type=F32)
            dk_s[...] += jnp.dot(ds, queries, preferred_element_type=F32)
            dq_s[at, :] = jnp.dot(knt_s[...], ds, preferred_element_type=F32).T * factor
            return carry

        lax.fori_loop(0, length // block, visit, 0)
        dq, part = rms_backward(triple[:, columns(0, h)].astype(F32), query_gain, dq_s[...])
        gain_q += part
        grads[:, columns(0, h)] = dq.astype(BF16)
        dk, part = rms_backward(
            triple[:, columns(1, h)].astype(F32), key_gain, dk_s[...] * factor
        )
        gain_k += part
        grads[:, columns(1, h)] = dk.astype(BF16)
        grads[:, columns(2, h)] = dv_s[...].astype(BF16)

    gain_all[s, 0:1, :] = gain_q
    gain_all[s, 1:2, :] = gain_k
    for k in range(1, ns):
        launch(
            remote(
                gain_all.at[s], gain_all.at[s], g_send.at[k], g_recv.at[s],
                (f, lax.rem(s + k, ns)),
            )
        )

    def text_at(index):
        return pl.ds(pl.multiple_of(index * piece, piece), piece)

    def share(at):
        return lax.dot_general(grads[at, :], weights[...], NT, preferred_element_type=F32)

    text_share[...] = share(pl.ds(0, text_rows))
    cuts = ((0, piece + chunk), (piece + chunk, rows - chunk))
    ends = (z == 0) | (z == nz - 1)
    middle = (z > 0) & (z < nz - 1)

    def ordered(k):
        return jnp.where(2 * z < nz, nz - 1 - k, k)

    def fill(k):
        zt = ordered(k)
        value = share(pl.ds(place(z, zt, 0), pair))
        low, high = value[:rows], value[rows:]
        here = core == 0
        mine[zt, pl.ds(piece, rows), :] = jnp.where(here, low, high)
        mine[zt, pl.ds(0, piece), :] = text_share[text_at(zt * 2 + core), :]
        sib_send[zt, pl.ds(piece, rows), :] = jnp.where(here, high, low).astype(BF16)
        sib_send[zt, pl.ds(0, piece), :] = text_share[text_at(zt * 2 + other), :].astype(BF16)
        launch(
            remote(sib_send.at[zt], sib_recv.at[zt], sb_send.at[zt], sb_recv.at[zt], (f, sib))
        )

    def sib_wait(zt):
        remote(
            sib_send.at[zt], sib_recv.at[zt], sb_send.at[zt], sb_recv.at[zt], (f, s)
        ).wait_recv()

    def combined(zt, cut):
        at = pl.ds(*cut)
        return mine[zt, at, :] + sib_recv[zt, at, :].astype(F32)

    def line_copy(zt, ch, to_z):
        slot = jnp.where((to_z < z) & (zt == to_z), nz, zt)
        at = pl.ds(*cuts[ch])
        return remote(
            line_send.at[zt, at], line_recv.at[slot, at], zs_send.at[zt, ch],
            zs_recv.at[slot, ch], (f, to_z * 2 + core),
        )

    def line_wait(slot, ch):
        at = pl.ds(*cuts[ch])
        remote(
            line_send.at[0, at], line_recv.at[slot, at], zs_send.at[0, ch],
            zs_recv.at[slot, ch], (f, s),
        ).wait_recv()

    def originate(k):
        zt = ordered(k)
        sib_wait(zt)
        for ch in range(CHUNKS):
            line_send[zt, pl.ds(*cuts[ch]), :] = combined(zt, cuts[ch]).astype(BF16)
            line_copy(zt, ch, jnp.where(z == 0, 1, nz - 2)).start()

    def pass_on(zt, ch, to_z):
        at = pl.ds(*cuts[ch])
        line_wait(zt, ch)
        total = combined(zt, cuts[ch]) + line_recv[zt, at, :].astype(F32)
        line_send[zt, at, :] = total.astype(BF16)
        line_copy(zt, ch, to_z).start()

    targets = [partner] + peers + corners

    def term(k):
        target = f if k == nf - 1 else targets[k]
        value = jnp.dot(tokens_t[w_at(target), :], grads[...], preferred_element_type=F32)
        if k < nf - 1:
            w_send[k] = value.astype(BF16)
            launch(
                remote(w_send.at[k], w_recv.at[f], ws_send.at[k], ws_recv.at[f], (target, s))
            )
        else:
            rounded = value.astype(BF16).astype(F32)
            for c in range(parts):
                weight_out[c] = rounded[:, c * own_width : (c + 1) * own_width]

    fill(0)
    for k in range(1, nz):
        fill(k)
        pl.when(ends)(functools.partial(originate, k - 1))
        if k <= nf:
            term(k - 1)
    for k in range(nz - 1, nf):
        term(k)

    for k in range(1, ns):
        source = lax.rem(s - k + ns, ns)
        remote(
            gain_all.at[source], gain_all.at[source], g_send.at[k], g_recv.at[source], (f, s)
        ).wait_recv()
    gain = gain_all[0]
    for i in range(1, ns):
        gain += gain_all[i]
    gain_rows[f] = gain
    for k in range(1, nf):
        launch(
            remote(
                gain_rows.at[f], gain_rows.at[f], h_send.at[k], h_recv.at[f],
                (lax.rem(f + k, nf), s),
            )
        )

    @pl.when(middle)
    def _():
        for k in range(nz):
            sib_wait(ordered(k))
        for t in range(nz - 1):
            for ch in range(CHUNKS):
                down = t - (nz - 1) + z
                pl.when(down >= 0)(functools.partial(pass_on, down, ch, z - 1))
                pl.when(t >= z)(functools.partial(pass_on, nz - 1 + z - t, ch, z + 1))

    pl.when(ends)(functools.partial(sib_wait, z))

    def finish(ch):
        at = pl.ds(*cuts[ch])

        def arrived(slot):
            line_wait(slot, ch)
            mine[z, at, :] += line_recv[slot, at, :].astype(F32)

        pl.when(down_ok)(functools.partial(arrived, z))
        pl.when(up_ok)(functools.partial(arrived, nz))
        total = combined(z, cuts[ch]).astype(BF16)
        if ch == 0:
            text_out[text_at(s), :] = total[:piece]
            image_out[pl.ds(0, chunk), :] = total[piece:]
        else:
            image_out[pl.ds(chunk, rows - chunk), :] = total

    t_count = []

    def t_launch(index, to_z, to_core):
        at = text_at(index)
        copy = remote(
            text_out.at[at], text_out.at[at], t_send.at[len(t_count)], t_recv.at[index],
            (f, to_z * 2 + to_core),
        )
        t_count.append(0)
        launch(copy)

    def t_wait(index):
        at = text_at(index)
        remote(
            text_out.at[at], text_out.at[at], t_send.at[0], t_recv.at[index], (f, s)
        ).wait_recv()

    finish(0)
    for k in range(1, nz):
        t_launch(s, lax.rem(z + k, nz), core)
    t_launch(s, z, other)

    for q in targets:
        remote(
            w_send.at[0], w_recv.at[q], ws_send.at[0], ws_recv.at[q], (f, s)
        ).wait_recv()
        for c in range(parts):
            weight_out[c] += w_recv[q, :, c * own_width : (c + 1) * own_width].astype(F32)
    for k in range(1, nf):
        source = lax.rem(f - k + nf, nf)
        remote(
            gain_rows.at[source], gain_rows.at[source], h_send.at[k], h_recv.at[source], (f, s)
        ).wait_recv()
    gain = gain_rows[0]
    for i in range(1, nf):
        gain += gain_rows[i]
    gain_out[...] = gain[:2]

    for k in range(1, nz):
        near = lax.rem(z - k + nz, nz) * 2 + core
        t_wait(near)
        t_launch(near, z, other)
    finish(1)
    for k in range(nz):
        t_wait(lax.rem(z + k, nz) * 2 + other)

    for where, copy in pending:
        if where is None:
            copy.wait_send()
        else:
            pl.when(where)(copy.wait_send)
    for ch in range(CHUNKS):
        for k in range(nz - 1):
            pl.when(ends)(line_copy(ordered(k), ch, jnp.where(z == 0, 1, nz - 2)).wait_send)

            def sent(zt, ch=ch):
                pl.when(zt != z)(line_copy(zt, ch, z).wait_send)

        for k in range(nz):
            pl.when(middle)(functools.partial(sent, k))


def emit(*refs):
    sems = refs[-1]
    count = len(refs) // 2
    copies = [
        pltpu.make_async_copy(refs[i], refs[count + i], sems.at[i]) for i in range(count)
    ]
    for copy in copies:
        copy.start()
    for copy in copies:
        copy.wait()


def local(nf, ns, image_input, text_input, w_qkv, query_gain, key_gain, image_up, text_up):
    _, rows, depth = image_input.shape
    text_rows = text_input.shape[1]
    w_rows, three, all_width = w_qkv.shape
    own_width = all_width // ns
    head = query_gain.shape[0]
    heads = own_width // head
    length = text_rows + rows * ns
    nz = ns // 2
    width3 = three * own_width
    tall = rows + text_rows // ns
    vmem = pl.BlockSpec(memory_space=pltpu.VMEM)
    hbm = pl.BlockSpec(memory_space=pl.ANY)
    dma = pltpu.SemaphoreType.DMA
    results = pl.pallas_call(
        functools.partial(kernel, nf, ns),
        out_shape=(
            pltpu.VMEM((rows, depth), BF16),
            pltpu.VMEM((text_rows, depth), BF16),
            pltpu.VMEM((three, w_rows, own_width), F32),
            pltpu.VMEM((2, head), F32),
        ),
        in_specs=[hbm, hbm, hbm, hbm, hbm, vmem, vmem],
        out_specs=(vmem,) * 4,
        scratch_shapes=[
            pltpu.VMEM((length, depth), BF16),
            pltpu.VMEM((depth, width3), BF16),
            pltpu.VMEM((length, own_width), BF16),
            pltpu.VMEM((length, width3), BF16),
            pltpu.VMEM((length, width3), BF16),
            pltpu.VMEM((length, head), BF16),
            pltpu.VMEM((length, head), BF16),
            pltpu.VMEM((head, length), BF16),
            pltpu.VMEM((length, head), F32),
            pltpu.VMEM((length, head), F32),
            pltpu.VMEM((length, head), F32),
            pltpu.VMEM((nz, tall, depth), BF16),
            pltpu.VMEM((nz, tall, depth), BF16),
            pltpu.VMEM((nz, tall, depth), F32),
            pltpu.VMEM((nz, tall, depth), BF16),
            pltpu.VMEM((nz + 1, tall, depth), BF16),
            pltpu.VMEM((nf - 1, w_rows, width3), BF16),
            pltpu.VMEM((nf, w_rows, width3), BF16),
            pltpu.VMEM((ns, 8, head), F32),
            pltpu.VMEM((nf, 8, head), F32),
            pltpu.VMEM((text_rows, depth), F32),
            pltpu.VMEM((depth, length), BF16),
            dma((3 * CHUNKS + 4 * (nz - 1) * CHUNKS,)), dma((ns, CHUNKS)),
            dma((heads * (1 + 4 * (nz - 1)),)), dma((heads, ns)),
            dma((2 + 4 * (nf // 2 - 1),)), dma((nf, 2)),
            dma((nz,)), dma((nz,)),
            dma((nz, CHUNKS)), dma((nz + 1, CHUNKS)),
            dma((nf,)), dma((nf,)),
            dma((ns,)), dma((ns,)),
            dma((nf,)), dma((nf,)),
            dma((2 * nz,)), dma((ns,)),
            dma((4 + three,)),
        ],
        compiler_params=pltpu.CompilerParams(
            collective_id=0, has_side_effects=True, vmem_limit_bytes=56 * 1024 * 1024
        ),
        name="joint_backward",
    )(
        image_input[0], text_input[0], w_qkv.transpose(1, 0, 2), image_up[0], text_up[0],
        query_gain.reshape(1, head), key_gain.reshape(1, head),
    )
    image_grad, text_grad, weight_grad, gain = pl.pallas_call(
        emit,
        out_shape=tuple(jax.ShapeDtypeStruct(r.shape, r.dtype) for r in results),
        in_specs=[hbm] * 4,
        out_specs=(hbm,) * 4,
        scratch_shapes=[dma((4,))],
        compiler_params=pltpu.CompilerParams(vmem_limit_bytes=1024 * 1024),
        name="emit",
    )(*results)
    return (
        image_grad[None],
        text_grad[None],
        weight_grad.transpose(1, 0, 2),
        gain,
    )


def solution(mesh):
    return jax.shard_map(
        functools.partial(local, mesh.shape["fsdp"], mesh.shape["seq"]),
        mesh=mesh,
        in_specs=(
            P("fsdp", "seq", None),
            P("fsdp", None, None),
            P("fsdp", None, None),
            P(),
            P(),
            P("fsdp", "seq", None),
            P("fsdp", None, None),
        ),
        out_specs=(P("fsdp", "seq", None), P("fsdp", None, None), P("fsdp", None, "seq"), P()),
        check_vma=False,
    )
```

```python
import functools
import math

import jax
import jax.numpy as jnp
from jax import lax
from jax.experimental import pallas as pl
from jax.experimental.pallas import tpu as pltpu
from jax.sharding import PartitionSpec as P

EPSILON = 1e-06
MESH = pl.DeviceIdType.MESH
F32 = jnp.float32
BF16 = jnp.bfloat16
NT = (((1,), (1,)), ((), ()))
CHUNKS = 2


def kernel(
    nf, ns, image_ref, text_ref, weight_ref, up_ref, text_up_ref, qg_ref, kg_ref,
    image_out, text_out, weight_out, gain_out,
    tokens, weights, ups, triple, grads, qn_s, kn_s, knt_s, dq_s, dk_s, dv_s,
    sib_send, sib_recv, mine, line_send, line_recv, w_send, w_recv, gain_all, gain_rows,
    text_share, text_sib_send, text_sib_recv, text_send, text_recv, tokens_t,
    x_send, x_recv, u_send, u_recv, wg_send, wg_recv, sb_send, sb_recv,
    zs_send, zs_recv, ws_send, ws_recv, g_send, g_recv, h_send, h_recv, t_send, t_recv,
    ts_send, ts_recv, tz_send, tz_recv, l_sem,
):
    f = lax.axis_index("fsdp")
    s = lax.axis_index("seq")
    nz = ns // 2
    z = lax.div(s, 2)
    core = lax.rem(s, 2)
    other = 1 - core
    sib = z * 2 + other
    rows = image_ref.shape[0]
    text_rows = text_ref.shape[0]
    parts, w_rows, all_width = weight_ref.shape
    own_width = all_width // ns
    head = qg_ref.shape[1]
    heads = own_width // head
    length = tokens.shape[0]
    piece = text_rows // 4
    chunk = rows // CHUNKS
    half = w_rows // 2
    pending = []

    def remote(src, dst, send, recv, target):
        return pltpu.make_async_remote_copy(
            src_ref=src, dst_ref=dst, send_sem=send, recv_sem=recv,
            device_id=target, device_id_type=MESH,
        )

    def launch(copy, where=None):
        if where is None:
            copy.start()
        else:
            pl.when(where)(copy.start)
        pending.append((where, copy))

    def rank(at, who):
        away = jnp.abs(who - at)
        nearer = jnp.minimum(away - 1, at) + jnp.minimum(away - 1, nz - 1 - at)
        second = jnp.where((who > at) & (at >= away), 1, 0)
        return jnp.where(away == 0, 0, 1 + nearer + second)

    def place(at, who, which):
        return pl.multiple_of(text_rows + (rank(at, who) * 2 + which) * rows, rows)

    def w_at(index):
        return pl.ds(pl.multiple_of(index * w_rows, w_rows), w_rows)

    def u_at(index):
        return pl.ds(pl.multiple_of(index * own_width, own_width), own_width)

    own_at = pl.ds(place(z, z, core), rows)
    locals_ = [
        pltpu.make_async_copy(
            weight_ref.at[c, :, u_at(s)],
            weights.at[w_at(f), pl.ds(c * own_width, own_width)],
            l_sem.at[4 + c],
        )
        for c in range(parts)
    ] + [
        pltpu.make_async_copy(image_ref, tokens.at[own_at], l_sem.at[0]),
        pltpu.make_async_copy(text_ref, tokens.at[pl.ds(0, text_rows)], l_sem.at[1]),
        pltpu.make_async_copy(up_ref.at[:, u_at(s)], ups.at[own_at], l_sem.at[2]),
        pltpu.make_async_copy(
            text_up_ref.at[:, u_at(s)], ups.at[pl.ds(0, text_rows)], l_sem.at[3]
        ),
    ]
    for copy in locals_:
        copy.start()

    barrier = pltpu.get_barrier_semaphore()
    for k in range(1, nf):
        pl.semaphore_signal(
            barrier, inc=1, device_id=(lax.rem(f + k, nf), s), device_id_type=MESH
        )
    for k in range(1, ns):
        pl.semaphore_signal(
            barrier, inc=1, device_id=(f, lax.rem(s + k, ns)), device_id_type=MESH
        )
    pl.semaphore_wait(barrier, nf + ns - 2)

    up_ok = z < nz - 1
    down_ok = z > 0

    def x_copy(source, which, ch, to_z, to_core, own=False):
        src = (
            image_ref.at[pl.ds(ch * chunk, chunk)]
            if own
            else tokens.at[pl.ds(place(z, source, which) + ch * chunk, chunk)]
        )
        return remote(
            src,
            tokens.at[pl.ds(place(to_z, source, which) + ch * chunk, chunk)],
            x_send.at[len(x_count)],
            x_recv.at[rank(to_z, source) * 2 + which, ch],
            (f, to_z * 2 + to_core),
        )

    x_count = []

    def x_launch(*args, where=None, **kw):
        copy = x_copy(*args, **kw)
        x_count.append(0)
        launch(copy, where)

    def x_wait(source, which, ch):
        remote(
            image_ref.at[pl.ds(0, chunk)],
            tokens.at[pl.ds(place(z, source, which) + ch * chunk, chunk)],
            x_send.at[0], x_recv.at[rank(z, source) * 2 + which, ch], (f, s),
        ).wait_recv()

    for ch in range(CHUNKS):
        x_launch(z, core, ch, z + 1, core, own=True, where=up_ok)
        x_launch(z, core, ch, z - 1, core, own=True, where=down_ok)
        x_launch(z, core, ch, z, other, own=True)

    fast = lax.rem(f, 2)
    slow = lax.div(f, 2)
    na = nf // 2
    partner = slow * 2 + 1 - fast
    around = [lax.rem(slow + j, na) for j in range(1, na)]
    peers = [a * 2 + fast for a in around]
    corners = [a * 2 + 1 - fast for a in around]

    def w_half(source, hf):
        return weights.at[pl.ds(pl.multiple_of(source * w_rows + hf * half, half), half)]

    w_count = []

    def w_launch(source, hf, target):
        copy = remote(
            w_half(source, hf), w_half(source, hf), wg_send.at[len(w_count)],
            wg_recv.at[source, hf], (target, s),
        )
        w_count.append(0)
        launch(copy)

    def w_wait(source, hf):
        remote(
            w_half(f, hf), w_half(source, hf), wg_send.at[0], wg_recv.at[source, hf], (f, s)
        ).wait_recv()

    for copy in locals_[:parts]:
        copy.wait()
    w_launch(f, 0, partner)
    for q in peers:
        w_launch(f, 1, q)
    w_launch(f, 1, partner)
    for q in peers:
        w_launch(f, 0, q)
    for copy in locals_[parts:]:
        copy.wait()

    def relay_weights():
        w_wait(partner, 0)
        for q in peers:
            w_launch(partner, 0, q)
        for q in peers:
            w_wait(q, 1)
            w_launch(q, 1, partner)

    def finish_weights():
        w_wait(partner, 1)
        for q in peers:
            w_wait(q, 0)
        for q in corners:
            w_wait(q, 0)
            w_wait(q, 1)

    u_count = []

    def u_launch(to_z, to_core, h, where=None):
        column = (to_z * 2 + to_core) * own_width + h * head
        copy = remote(
            up_ref.at[:, pl.ds(pl.multiple_of(column, head), head)],
            ups.at[pl.ds(place(to_z, z, core), rows), pl.ds(h * head, head)],
            u_send.at[len(u_count)],
            u_recv.at[h, rank(to_z, z) * 2 + core],
            (f, to_z * 2 + to_core),
        )
        u_count.append(0)
        launch(copy, where)

    def send_upstream():
        for h in range(heads):
            u_launch(z, other, h)
            for d in range(1, nz):
                for which in (core, other):
                    u_launch(z + d, which, h, where=z + d < nz)
                    u_launch(z - d, which, h, where=z - d >= 0)

    def transpose(start, count):
        at = pl.ds(start, count)
        tokens_t[:, at] = tokens[at, :].T

    def project(start, count):
        at = pl.ds(start, count)
        triple[at, :] = jnp.dot(
            tokens[at, :], weights[...], preferred_element_type=F32
        ).astype(BF16)

    pair = 2 * rows
    first = text_rows + pair
    relayed = False
    for d in range(1, nz):
        sides = (
            (z - d, z - d >= 0, z + 1, up_ok),
            (z + d, z + d < nz, z - 1, down_ok),
        )
        if d == nz - 1:
            if not relayed:
                relay_weights()
                relayed = True
            for ch in range(CHUNKS):
                x_wait(z, other, ch)
            transpose(0, first)
            for k in range(1, nz - 1):
                transpose(first + (k - 1) * pair, pair)
            finish_weights()
            project(0, first)
            for k in range(1, nz - 1):
                project(first + (k - 1) * pair, pair)
        for ch in range(CHUNKS):
            for source, exists, onward, onward_ok in sides:
                pl.when(exists)(functools.partial(x_wait, source, core, ch))
                x_launch(source, core, ch, onward, core, where=exists & onward_ok)
                x_launch(source, core, ch, z, other, where=exists)
            if not relayed:
                relay_weights()
                relayed = True
        for ch in range(CHUNKS):
            for source, exists, onward, onward_ok in sides:
                pl.when(exists)(functools.partial(x_wait, source, other, ch))
        if d == max(1, nz - 2):
            send_upstream()
    last = first + (nz - 2) * pair
    transpose(last, pair)
    project(last, pair)

    factor = 1.0 / math.sqrt(head)
    query_gain = qg_ref[...]
    key_gain = kg_ref[...]
    block = max(b for b in range(128, 385, 128) if length % b == 0)
    per_block = block // rows
    text_pieces = text_rows // rows

    def columns(c, h):
        return pl.ds(c * own_width + h * head, head)

    def inverse_of(values):
        return lax.rsqrt(jnp.mean(values * values, axis=-1, keepdims=True) + EPSILON)

    def rms_backward(values, gain, incoming):
        inverse = inverse_of(values)
        weighted = incoming * gain
        inner = jnp.mean(weighted * values, axis=-1, keepdims=True)
        grad = inverse * weighted - values * (inverse * inverse * inverse * inner)
        return grad, jnp.sum(incoming * values * inverse, axis=0, keepdims=True)

    def u_wait(h, j):
        at = pl.ds(pl.multiple_of(text_rows + j * rows, rows), rows)
        remote(
            up_ref.at[:, pl.ds(0, head)],
            ups.at[at, pl.ds(h * head, head)],
            u_send.at[0], u_recv.at[h, j], (f, s),
        ).wait_recv()

    gain_q = jnp.zeros((1, head), F32)
    gain_k = jnp.zeros((1, head), F32)
    for h in range(heads):
        qf = triple[:, columns(0, h)].astype(F32)
        qn_s[...] = (qf * inverse_of(qf) * query_gain).astype(BF16)
        kf = triple[:, columns(1, h)].astype(F32)
        kn = (kf * inverse_of(kf) * key_gain).astype(BF16)
        kn_s[...] = kn
        knt_s[...] = kn.astype(F32).T.astype(BF16)
        dk_s[...] = jnp.zeros_like(dk_s)
        dv_s[...] = jnp.zeros_like(dv_s)

        def visit(i, carry, h=h):
            for jj in range(per_block):
                j = i * per_block + jj - text_pieces
                pl.when((j >= 0) & (j != core))(functools.partial(u_wait, h, j))
            at = pl.ds(pl.multiple_of(i * block, block), block)
            queries = qn_s[at, :]
            upstream = ups[at, pl.ds(h * head, head)]
            scores = lax.dot_general(kn_s[...], queries, NT, preferred_element_type=F32)
            p = jnp.exp(scores * factor)
            p = p * (1.0 / jnp.sum(p, axis=0, keepdims=True))
            dp = lax.dot_general(
                triple[:, columns(2, h)], upstream, NT, preferred_element_type=F32
            )
            dot = jnp.sum(p * dp, axis=0, keepdims=True)
            ds = (p * (dp - dot)).astype(BF16)
            dv_s[...] += jnp.dot(p.astype(BF16), upstream, preferred_element_type=F32)
            dk_s[...] += jnp.dot(ds, queries, preferred_element_type=F32)
            dq_s[at, :] = jnp.dot(knt_s[...], ds, preferred_element_type=F32).T * factor
            return carry

        lax.fori_loop(0, length // block, visit, 0)
        dq, part = rms_backward(triple[:, columns(0, h)].astype(F32), query_gain, dq_s[...])
        gain_q += part
        grads[:, columns(0, h)] = dq.astype(BF16)
        dk, part = rms_backward(
            triple[:, columns(1, h)].astype(F32), key_gain, dk_s[...] * factor
        )
        gain_k += part
        grads[:, columns(1, h)] = dk.astype(BF16)
        grads[:, columns(2, h)] = dv_s[...].astype(BF16)

    gain_all[s, 0:1, :] = gain_q
    gain_all[s, 1:2, :] = gain_k
    for k in range(1, ns):
        launch(
            remote(
                gain_all.at[s], gain_all.at[s], g_send.at[k], g_recv.at[s],
                (f, lax.rem(s + k, ns)),
            )
        )

    def text_at(index):
        return pl.ds(pl.multiple_of(index * piece, piece), piece)

    def share(at):
        return lax.dot_general(grads[at, :], weights[...], NT, preferred_element_type=F32)

    text_share[...] = share(pl.ds(0, text_rows))
    cuts = [(ch * chunk, chunk) for ch in range(CHUNKS)]
    ends = (z == 0) | (z == nz - 1)
    middle = (z > 0) & (z < nz - 1)

    def ordered(k):
        return jnp.where(2 * z < nz, nz - 1 - k, k)

    def text_swap():
        for o in range(2):
            text_sib_send[o] = text_share[text_at(o * 2 + other), :].astype(BF16)
        return remote(
            text_sib_send, text_sib_recv, ts_send.at[0], ts_recv.at[0], (f, sib)
        )

    swap = text_swap()
    launch(swap)

    def text_line(o, direction):
        return remote(
            text_send.at[o], text_recv.at[1 - direction, o], tz_send.at[o],
            tz_recv.at[1 - direction, o], (f, (z - 1 + 2 * direction) * 2 + core),
        )

    def t_copy(index, to_z, to_core, slot):
        at = text_at(index)
        return remote(
            text_out.at[at], text_out.at[at], t_send.at[slot], t_recv.at[index],
            (f, to_z * 2 + to_core),
        )

    def own_text():
        index = (z - (nz // 2 - 1)) * 2 + core
        copies = [t_copy(index, lax.rem(z + k, nz), core, k) for k in range(1, nz)]
        return copies + [t_copy(index, z, other, 0)]

    def text_step(k):
        o = jnp.where(2 * z < nz, 1 - k, k)
        owner = nz // 2 - 1 + o
        at = text_at(o * 2 + core)
        text_share[at, :] += text_sib_recv[o].astype(F32)

        def arrived(side):
            remote(
                text_send.at[0], text_recv.at[side, o], tz_send.at[0], tz_recv.at[side, o],
                (f, s),
            ).wait_recv()
            text_share[at, :] += text_recv[side, o].astype(F32)

        pl.when((z > 0) & (z <= owner))(functools.partial(arrived, 0))
        pl.when((z < nz - 1) & (z >= owner))(functools.partial(arrived, 1))
        total = text_share[at, :].astype(BF16)

        @pl.when(z != owner)
        def _():
            text_send[o] = total
            text_line(o, jnp.where(z < owner, 1, 0)).start()

        @pl.when(z == owner)
        def _():
            text_out[at, :] = total
            for copy in own_text():
                copy.start()

    def text_steps():
        swap.wait_recv()
        for k in range(2):
            text_step(k)

    def fill(k):
        zt = ordered(k)
        value = share(pl.ds(place(z, zt, 0), pair))
        low, high = value[:rows], value[rows:]
        here = core == 0
        mine[zt] = jnp.where(here, low, high)
        sib_send[zt] = jnp.where(here, high, low).astype(BF16)
        launch(
            remote(sib_send.at[zt], sib_recv.at[zt], sb_send.at[zt], sb_recv.at[zt], (f, sib))
        )

    def sib_wait(zt):
        remote(
            sib_send.at[zt], sib_recv.at[zt], sb_send.at[zt], sb_recv.at[zt], (f, s)
        ).wait_recv()

    def combined(zt, cut):
        at = pl.ds(*cut)
        return mine[zt, at, :] + sib_recv[zt, at, :].astype(F32)

    def line_copy(zt, ch, to_z):
        slot = jnp.where((to_z < z) & (zt == to_z), nz, zt)
        at = pl.ds(*cuts[ch])
        return remote(
            line_send.at[zt, at], line_recv.at[slot, at], zs_send.at[zt, ch],
            zs_recv.at[slot, ch], (f, to_z * 2 + core),
        )

    def line_wait(slot, ch):
        at = pl.ds(*cuts[ch])
        remote(
            line_send.at[0, at], line_recv.at[slot, at], zs_send.at[0, ch],
            zs_recv.at[slot, ch], (f, s),
        ).wait_recv()

    def originate(k):
        zt = ordered(k)
        sib_wait(zt)
        for ch in range(CHUNKS):
            line_send[zt, pl.ds(*cuts[ch]), :] = combined(zt, cuts[ch]).astype(BF16)
            line_copy(zt, ch, jnp.where(z == 0, 1, nz - 2)).start()

    def pass_on(zt, ch, to_z):
        at = pl.ds(*cuts[ch])
        line_wait(zt, ch)
        total = combined(zt, cuts[ch]) + line_recv[zt, at, :].astype(F32)
        line_send[zt, at, :] = total.astype(BF16)
        line_copy(zt, ch, to_z).start()

    targets = [partner] + peers + corners

    def term(k):
        target = f if k == nf - 1 else targets[k]
        value = jnp.dot(tokens_t[w_at(target), :], grads[...], preferred_element_type=F32)
        if k < nf - 1:
            w_send[k] = value.astype(BF16)
            launch(
                remote(w_send.at[k], w_recv.at[f], ws_send.at[k], ws_recv.at[f], (target, s))
            )
        else:
            rounded = value.astype(BF16).astype(F32)
            for c in range(parts):
                weight_out[c] = rounded[:, c * own_width : (c + 1) * own_width]

    fill(0)
    pl.when(ends)(text_steps)
    for k in range(1, nz):
        fill(k)
        pl.when(ends)(functools.partial(originate, k - 1))
        if k <= nf:
            term(k - 1)
    for k in range(nz - 1, nf):
        term(k)

    for k in range(1, ns):
        source = lax.rem(s - k + ns, ns)
        remote(
            gain_all.at[source], gain_all.at[source], g_send.at[k], g_recv.at[source], (f, s)
        ).wait_recv()
    gain = gain_all[0]
    for i in range(1, ns):
        gain += gain_all[i]
    gain_rows[f] = gain
    for k in range(1, nf):
        launch(
            remote(
                gain_rows.at[f], gain_rows.at[f], h_send.at[k], h_recv.at[f],
                (lax.rem(f + k, nf), s),
            )
        )

    @pl.when(middle)
    def _():
        text_steps()
        for k in range(nz):
            sib_wait(ordered(k))
        for t in range(nz - 1):
            for ch in range(CHUNKS):
                down = t - (nz - 1) + z
                pl.when(down >= 0)(functools.partial(pass_on, down, ch, z - 1))
                pl.when(t >= z)(functools.partial(pass_on, nz - 1 + z - t, ch, z + 1))

    pl.when(ends)(functools.partial(sib_wait, z))

    def finish(ch):
        at = pl.ds(*cuts[ch])

        def arrived(slot):
            line_wait(slot, ch)
            mine[z, at, :] += line_recv[slot, at, :].astype(F32)

        pl.when(down_ok)(functools.partial(arrived, z))
        pl.when(up_ok)(functools.partial(arrived, nz))
        image_out[at, :] = combined(z, cuts[ch]).astype(BF16)

    def t_wait(index):
        t_copy(index, z, core, 0).wait_recv()

    center = nz // 2 - 1
    for o in range(2):
        index = o * 2 + core

        @pl.when(z != center + o)
        def _(index=index, o=o):
            t_wait(index)
            t_copy(index, z, other, nz + o).start()

    finish(0)
    for q in targets:
        remote(
            w_send.at[0], w_recv.at[q], ws_send.at[0], ws_recv.at[q], (f, s)
        ).wait_recv()
        for c in range(parts):
            weight_out[c] += w_recv[q, :, c * own_width : (c + 1) * own_width].astype(F32)
    for k in range(1, nf):
        source = lax.rem(f - k + nf, nf)
        remote(
            gain_rows.at[source], gain_rows.at[source], h_send.at[k], h_recv.at[source], (f, s)
        ).wait_recv()
    gain = gain_rows[0]
    for i in range(1, nf):
        gain += gain_rows[i]
    gain_out[...] = gain[:2]

    for ch in range(1, CHUNKS):
        finish(ch)
    for o in range(2):
        t_wait(o * 2 + other)

    for where, copy in pending:
        if where is None:
            copy.wait_send()
        else:
            pl.when(where)(copy.wait_send)
    for ch in range(CHUNKS):
        for k in range(nz - 1):
            pl.when(ends)(line_copy(ordered(k), ch, jnp.where(z == 0, 1, nz - 2)).wait_send)

            def sent(zt, ch=ch):
                pl.when(zt != z)(line_copy(zt, ch, z).wait_send)

        for k in range(nz):
            pl.when(middle)(functools.partial(sent, k))
    for o in range(2):
        owner = center + o
        pl.when(z != owner)(text_line(o, jnp.where(z < owner, 1, 0)).wait_send)
        pl.when(z != owner)(t_copy(o * 2 + core, z, other, nz + o).wait_send)

    @pl.when((z == center) | (z == center + 1))
    def _():
        for copy in own_text():
            copy.wait_send()


def emit(*refs):
    sems = refs[-1]
    count = len(refs) // 2
    copies = [
        pltpu.make_async_copy(refs[i], refs[count + i], sems.at[i]) for i in range(count)
    ]
    for copy in copies:
        copy.start()
    for copy in copies:
        copy.wait()


def local(nf, ns, image_input, text_input, w_qkv, query_gain, key_gain, image_up, text_up):
    _, rows, depth = image_input.shape
    text_rows = text_input.shape[1]
    w_rows, three, all_width = w_qkv.shape
    own_width = all_width // ns
    head = query_gain.shape[0]
    heads = own_width // head
    length = text_rows + rows * ns
    nz = ns // 2
    width3 = three * own_width
    piece = text_rows // 4
    vmem = pl.BlockSpec(memory_space=pltpu.VMEM)
    hbm = pl.BlockSpec(memory_space=pl.ANY)
    dma = pltpu.SemaphoreType.DMA
    results = pl.pallas_call(
        functools.partial(kernel, nf, ns),
        out_shape=(
            pltpu.VMEM((rows, depth), BF16),
            pltpu.VMEM((text_rows, depth), BF16),
            pltpu.VMEM((three, w_rows, own_width), F32),
            pltpu.VMEM((2, head), F32),
        ),
        in_specs=[hbm, hbm, hbm, hbm, hbm, vmem, vmem],
        out_specs=(vmem,) * 4,
        scratch_shapes=[
            pltpu.VMEM((length, depth), BF16),
            pltpu.VMEM((depth, width3), BF16),
            pltpu.VMEM((length, own_width), BF16),
            pltpu.VMEM((length, width3), BF16),
            pltpu.VMEM((length, width3), BF16),
            pltpu.VMEM((length, head), BF16),
            pltpu.VMEM((length, head), BF16),
            pltpu.VMEM((head, length), BF16),
            pltpu.VMEM((length, head), F32),
            pltpu.VMEM((length, head), F32),
            pltpu.VMEM((length, head), F32),
            pltpu.VMEM((nz, rows, depth), BF16),
            pltpu.VMEM((nz, rows, depth), BF16),
            pltpu.VMEM((nz, rows, depth), F32),
            pltpu.VMEM((nz, rows, depth), BF16),
            pltpu.VMEM((nz + 1, rows, depth), BF16),
            pltpu.VMEM((nf - 1, w_rows, width3), BF16),
            pltpu.VMEM((nf, w_rows, width3), BF16),
            pltpu.VMEM((ns, 8, head), F32),
            pltpu.VMEM((nf, 8, head), F32),
            pltpu.VMEM((text_rows, depth), F32),
            pltpu.VMEM((2, piece, depth), BF16),
            pltpu.VMEM((2, piece, depth), BF16),
            pltpu.VMEM((2, piece, depth), BF16),
            pltpu.VMEM((2, 2, piece, depth), BF16),
            pltpu.VMEM((depth, length), BF16),
            dma((3 * CHUNKS + 4 * (nz - 1) * CHUNKS,)), dma((ns, CHUNKS)),
            dma((heads * (1 + 4 * (nz - 1)),)), dma((heads, ns)),
            dma((2 + 4 * (nf // 2 - 1),)), dma((nf, 2)),
            dma((nz,)), dma((nz,)),
            dma((nz, CHUNKS)), dma((nz + 1, CHUNKS)),
            dma((nf,)), dma((nf,)),
            dma((ns,)), dma((ns,)),
            dma((nf,)), dma((nf,)),
            dma((nz + 2,)), dma((4,)),
            dma((1,)), dma((1,)), dma((2,)), dma((2, 2)),
            dma((4 + three,)),
        ],
        compiler_params=pltpu.CompilerParams(
            collective_id=0, has_side_effects=True, vmem_limit_bytes=56 * 1024 * 1024
        ),
        name="joint_backward",
    )(
        image_input[0], text_input[0], w_qkv.transpose(1, 0, 2), image_up[0], text_up[0],
        query_gain.reshape(1, head), key_gain.reshape(1, head),
    )
    image_grad, text_grad, weight_grad, gain = pl.pallas_call(
        emit,
        out_shape=tuple(jax.ShapeDtypeStruct(r.shape, r.dtype) for r in results),
        in_specs=[hbm] * 4,
        out_specs=(hbm,) * 4,
        scratch_shapes=[dma((4,))],
        compiler_params=pltpu.CompilerParams(vmem_limit_bytes=1024 * 1024),
        name="emit",
    )(*results)
    return (
        image_grad[None],
        text_grad[None],
        weight_grad.transpose(1, 0, 2),
        gain,
    )


def solution(mesh):
    return jax.shard_map(
        functools.partial(local, mesh.shape["fsdp"], mesh.shape["seq"]),
        mesh=mesh,
        in_specs=(
            P("fsdp", "seq", None),
            P("fsdp", None, None),
            P("fsdp", None, None),
            P(),
            P(),
            P("fsdp", "seq", None),
            P("fsdp", None, None),
        ),
        out_specs=(P("fsdp", "seq", None), P("fsdp", None, None), P("fsdp", None, "seq"), P()),
        check_vma=False,
    )
```

```python
import functools
import math

import jax
import jax.numpy as jnp
from jax import lax
from jax.experimental import pallas as pl
from jax.experimental.pallas import tpu as pltpu
from jax.sharding import PartitionSpec as P

EPSILON = 1e-06
MESH = pl.DeviceIdType.MESH
F32 = jnp.float32
BF16 = jnp.bfloat16
NT = (((1,), (1,)), ((), ()))
CHUNKS = 2


def kernel(
    nf, ns, image_ref, text_ref, weight_ref, up_ref, text_up_ref, qg_ref, kg_ref,
    image_out, text_out, weight_out, gain_out,
    tokens, weights, ups, triple, grads, qn_s, kn_s, knt_s, dk_s, dv_s, e_s, dp_s, p_s, ds_s,
    sib_send, sib_recv, mine, line_send, line_recv, w_send, w_recv, gain_all, gain_rows,
    text_share, text_sib_send, text_sib_recv, text_send, text_recv, tokens_t,
    x_send, x_recv, u_send, u_recv, wg_send, wg_recv, sb_send, sb_recv,
    zs_send, zs_recv, ws_send, ws_recv, g_send, g_recv, h_send, h_recv, t_send, t_recv,
    ts_send, ts_recv, tz_send, tz_recv, l_sem,
):
    f = lax.axis_index("fsdp")
    s = lax.axis_index("seq")
    nz = ns // 2
    z = lax.div(s, 2)
    core = lax.rem(s, 2)
    other = 1 - core
    sib = z * 2 + other
    rows = image_ref.shape[0]
    text_rows = text_ref.shape[0]
    parts, w_rows, all_width = weight_ref.shape
    own_width = all_width // ns
    head = qg_ref.shape[1]
    heads = own_width // head
    length = tokens.shape[0]
    piece = text_rows // 4
    chunk = rows // CHUNKS
    half = w_rows // 2
    pending = []

    def remote(src, dst, send, recv, target):
        return pltpu.make_async_remote_copy(
            src_ref=src, dst_ref=dst, send_sem=send, recv_sem=recv,
            device_id=target, device_id_type=MESH,
        )

    def launch(copy, where=None):
        if where is None:
            copy.start()
        else:
            pl.when(where)(copy.start)
        pending.append((where, copy))

    def rank(at, who):
        away = jnp.abs(who - at)
        nearer = jnp.minimum(away - 1, at) + jnp.minimum(away - 1, nz - 1 - at)
        second = jnp.where((who > at) & (at >= away), 1, 0)
        return jnp.where(away == 0, 0, 1 + nearer + second)

    def place(at, who, which):
        return pl.multiple_of(text_rows + (rank(at, who) * 2 + which) * rows, rows)

    def w_at(index):
        return pl.ds(pl.multiple_of(index * w_rows, w_rows), w_rows)

    def u_at(index):
        return pl.ds(pl.multiple_of(index * own_width, own_width), own_width)

    own_at = pl.ds(place(z, z, core), rows)
    locals_ = [
        pltpu.make_async_copy(
            weight_ref.at[c, :, u_at(s)],
            weights.at[w_at(f), pl.ds(c * own_width, own_width)],
            l_sem.at[4 + c],
        )
        for c in range(parts)
    ] + [
        pltpu.make_async_copy(image_ref, tokens.at[own_at], l_sem.at[0]),
        pltpu.make_async_copy(text_ref, tokens.at[pl.ds(0, text_rows)], l_sem.at[1]),
        pltpu.make_async_copy(up_ref.at[:, u_at(s)], ups.at[own_at], l_sem.at[2]),
        pltpu.make_async_copy(
            text_up_ref.at[:, u_at(s)], ups.at[pl.ds(0, text_rows)], l_sem.at[3]
        ),
    ]
    for copy in locals_:
        copy.start()

    barrier = pltpu.get_barrier_semaphore()
    for k in range(1, nf):
        pl.semaphore_signal(
            barrier, inc=1, device_id=(lax.rem(f + k, nf), s), device_id_type=MESH
        )
    for k in range(1, ns):
        pl.semaphore_signal(
            barrier, inc=1, device_id=(f, lax.rem(s + k, ns)), device_id_type=MESH
        )
    pl.semaphore_wait(barrier, nf + ns - 2)

    up_ok = z < nz - 1
    down_ok = z > 0

    def x_copy(source, which, ch, to_z, to_core, own=False):
        src = (
            image_ref.at[pl.ds(ch * chunk, chunk)]
            if own
            else tokens.at[pl.ds(place(z, source, which) + ch * chunk, chunk)]
        )
        return remote(
            src,
            tokens.at[pl.ds(place(to_z, source, which) + ch * chunk, chunk)],
            x_send.at[len(x_count)],
            x_recv.at[rank(to_z, source) * 2 + which, ch],
            (f, to_z * 2 + to_core),
        )

    x_count = []

    def x_launch(*args, where=None, **kw):
        copy = x_copy(*args, **kw)
        x_count.append(0)
        launch(copy, where)

    def x_wait(source, which, ch):
        remote(
            image_ref.at[pl.ds(0, chunk)],
            tokens.at[pl.ds(place(z, source, which) + ch * chunk, chunk)],
            x_send.at[0], x_recv.at[rank(z, source) * 2 + which, ch], (f, s),
        ).wait_recv()

    for ch in range(CHUNKS):
        x_launch(z, core, ch, z + 1, core, own=True, where=up_ok)
        x_launch(z, core, ch, z - 1, core, own=True, where=down_ok)
        x_launch(z, core, ch, z, other, own=True)

    fast = lax.rem(f, 2)
    slow = lax.div(f, 2)
    na = nf // 2
    partner = slow * 2 + 1 - fast
    around = [lax.rem(slow + j, na) for j in range(1, na)]
    peers = [a * 2 + fast for a in around]
    corners = [a * 2 + 1 - fast for a in around]

    def w_half(source, hf):
        return weights.at[pl.ds(pl.multiple_of(source * w_rows + hf * half, half), half)]

    w_count = []

    def w_launch(source, hf, target):
        copy = remote(
            w_half(source, hf), w_half(source, hf), wg_send.at[len(w_count)],
            wg_recv.at[source, hf], (target, s),
        )
        w_count.append(0)
        launch(copy)

    def w_wait(source, hf):
        remote(
            w_half(f, hf), w_half(source, hf), wg_send.at[0], wg_recv.at[source, hf], (f, s)
        ).wait_recv()

    for copy in locals_[:parts]:
        copy.wait()
    w_launch(f, 0, partner)
    for q in peers:
        w_launch(f, 1, q)
    w_launch(f, 1, partner)
    for q in peers:
        w_launch(f, 0, q)
    for copy in locals_[parts:]:
        copy.wait()

    def relay_weights():
        w_wait(partner, 0)
        for q in peers:
            w_launch(partner, 0, q)
        for q in peers:
            w_wait(q, 1)
            w_launch(q, 1, partner)

    def finish_weights():
        w_wait(partner, 1)
        for q in peers:
            w_wait(q, 0)
        for q in corners:
            w_wait(q, 0)
            w_wait(q, 1)

    def u_launch(to_z, to_core, h, slot, where=None):
        column = (to_z * 2 + to_core) * own_width + h * head
        copy = remote(
            up_ref.at[:, pl.ds(pl.multiple_of(column, head), head)],
            ups.at[pl.ds(place(to_z, z, core), rows), pl.ds(h * head, head)],
            u_send.at[h, slot],
            u_recv.at[h, rank(to_z, z) * 2 + core],
            (f, to_z * 2 + to_core),
        )
        launch(copy, where)

    def send_upstream(late):
        for h in range(heads):
            if not late:
                u_launch(z, other, h, 0)
            for d in range(1, nz):
                for to_z, exists, side in ((z + d, z + d < nz, 0), (z - d, z - d >= 0, 2)):
                    if d > 1:
                        outer = (to_z == 0) | (to_z == nz - 1)
                        exists = exists & (outer if late else ~outer)
                    elif late:
                        continue
                    for flip, which in enumerate((core, other)):
                        u_launch(to_z, which, h, 4 * d - 3 + side + flip, where=exists)

    factor = 1.0 / math.sqrt(head)
    query_gain = qg_ref[...]
    key_gain = kg_ref[...]
    block = e_s.shape[1]
    per_block = block // rows
    text_pieces = text_rows // rows

    def columns(c, h):
        return pl.ds(c * own_width + h * head, head)

    def inverse_of(values):
        return lax.rsqrt(jnp.mean(values * values, axis=-1, keepdims=True) + EPSILON)

    def transpose(start, count):
        at = pl.ds(start, count)
        tokens_t[:, at] = tokens[at, :].T

    def project(start, count):
        at = pl.ds(start, count)
        triple[at, :] = jnp.dot(
            tokens[at, :], weights[...], preferred_element_type=F32
        ).astype(BF16)
        for h in range(heads):
            for r in range(start, start + count, rows):
                at = pl.ds(r, rows)
                qf = triple[at, columns(0, h)].astype(F32)
                qn_s[h, at, :] = (qf * inverse_of(qf) * query_gain).astype(BF16)
                kf = triple[at, columns(1, h)].astype(F32)
                kn = kf * inverse_of(kf) * key_gain
                kn_s[h, at, :] = kn.astype(BF16)
                knt_s[h, :, at] = kn.T.astype(BF16)
                dk_s[h, at, :] = jnp.zeros((rows, head), F32)
                dv_s[h, at, :] = jnp.zeros((rows, head), F32)

    pair = 2 * rows
    first = text_rows + pair
    relayed = False
    for d in range(1, nz):
        sides = (
            (z - d, z - d >= 0, z + 1, up_ok),
            (z + d, z + d < nz, z - 1, down_ok),
        )
        if d == nz - 1:
            if not relayed:
                relay_weights()
                relayed = True
            for ch in range(CHUNKS):
                x_wait(z, other, ch)
            transpose(0, first)
            for k in range(1, nz - 1):
                transpose(first + (k - 1) * pair, pair)
            finish_weights()
            project(0, first)
            for k in range(1, nz - 1):
                project(first + (k - 1) * pair, pair)
        for ch in range(CHUNKS):
            for source, exists, onward, onward_ok in sides:
                pl.when(exists)(functools.partial(x_wait, source, core, ch))
                x_launch(source, core, ch, onward, core, where=exists & onward_ok)
                x_launch(source, core, ch, z, other, where=exists)
            if not relayed:
                relay_weights()
                relayed = True
        for ch in range(CHUNKS):
            for source, exists, onward, onward_ok in sides:
                pl.when(exists)(functools.partial(x_wait, source, other, ch))
        if d == max(1, nz - 2):
            send_upstream(False)
    send_upstream(True)
    last = first + (nz - 2) * pair
    transpose(last, pair)
    project(last, pair)

    def rms_backward(values, gain, incoming):
        inverse = inverse_of(values)
        weighted = incoming * gain
        inner = jnp.mean(weighted * values, axis=-1, keepdims=True)
        grad = inverse * weighted - values * (inverse * inverse * inverse * inner)
        return grad, jnp.sum(incoming * values * inverse, axis=0, keepdims=True)

    def u_wait(h, j):
        at = pl.ds(pl.multiple_of(text_rows + j * rows, rows), rows)
        remote(
            up_ref.at[:, pl.ds(0, head)],
            ups.at[at, pl.ds(h * head, head)],
            u_send.at[0, 0], u_recv.at[h, j], (f, s),
        ).wait_recv()

    scale = factor * math.log2(math.e)
    step = 128

    def folded(values):
        return jnp.sum(values.reshape(-1, 8, values.shape[1]), axis=0)

    gain_q = jnp.zeros((1, head), F32)
    gain_k = jnp.zeros((1, head), F32)
    for h in range(heads):
        def visit(i, carry, h=h):
            for jj in range(per_block):
                j = i * per_block + jj - text_pieces
                pl.when((j >= 0) & (j != core))(functools.partial(u_wait, h, j))
            at = pl.ds(pl.multiple_of(i * block, block), block)
            queries = qn_s[h, at, :]
            upstream = ups[at, pl.ds(h * head, head)]
            total = jnp.zeros((8, block), F32)
            dots = jnp.zeros((8, block), F32)
            for r in range(0, length, length):
                keys = pl.ds(r, length)
                scores = lax.dot_general(kn_s[h, keys, :], queries, NT, preferred_element_type=F32)
                e = jnp.exp2(scores * scale)
                e_s[keys, :] = e
                dp = lax.dot_general(
                    triple[keys, columns(2, h)], upstream, NT, preferred_element_type=F32
                )
                dp_s[keys, :] = dp
                total += folded(e)
                dots += folded(e * dp)
            inverse = 1.0 / jnp.sum(total, axis=0, keepdims=True)
            dot = jnp.sum(dots, axis=0, keepdims=True) * inverse
            for r in range(0, length, step):
                keys = pl.ds(r, step)
                p = e_s[keys, :] * inverse
                p_s[keys, :] = p.astype(BF16)
                ds_s[keys, :] = (p * (dp_s[keys, :] - dot)).astype(BF16)
            dv_s[h] += jnp.dot(p_s[...], upstream, preferred_element_type=F32)
            dk_s[h] += jnp.dot(ds_s[...], queries, preferred_element_type=F32)
            dqn = jnp.dot(knt_s[h], ds_s[...], preferred_element_type=F32).T * factor
            dq, part = rms_backward(triple[at, columns(0, h)].astype(F32), query_gain, dqn)
            grads[at, columns(0, h)] = dq.astype(BF16)
            return carry + part

        gain_q = lax.fori_loop(0, length // block, visit, gain_q)
        for r in range(0, length, step):
            at = pl.ds(r, step)
            dk, part = rms_backward(
                triple[at, columns(1, h)].astype(F32), key_gain, dk_s[h, at, :] * factor
            )
            gain_k += part
            grads[at, columns(1, h)] = dk.astype(BF16)
            grads[at, columns(2, h)] = dv_s[h, at, :].astype(BF16)

    early = len(pending)
    gain_all[s, 0:1, :] = gain_q
    gain_all[s, 1:2, :] = gain_k
    for k in range(1, ns):
        launch(
            remote(
                gain_all.at[s], gain_all.at[s], g_send.at[k], g_recv.at[s],
                (f, lax.rem(s + k, ns)),
            )
        )

    def text_at(index):
        return pl.ds(pl.multiple_of(index * piece, piece), piece)

    def share(at):
        return lax.dot_general(grads[at, :], weights[...], NT, preferred_element_type=F32)

    text_share[...] = share(pl.ds(0, text_rows))
    cuts = [(ch * chunk, chunk) for ch in range(CHUNKS)]
    ends = (z == 0) | (z == nz - 1)
    middle = (z > 0) & (z < nz - 1)

    def ordered(k):
        return jnp.where(2 * z < nz, nz - 1 - k, k)

    def text_swap():
        for o in range(2):
            text_sib_send[o] = text_share[text_at(o * 2 + other), :].astype(BF16)
        return remote(
            text_sib_send, text_sib_recv, ts_send.at[0], ts_recv.at[0], (f, sib)
        )

    swap = text_swap()
    launch(swap)

    def text_line(o, direction):
        return remote(
            text_send.at[o], text_recv.at[1 - direction, o], tz_send.at[o],
            tz_recv.at[1 - direction, o], (f, (z - 1 + 2 * direction) * 2 + core),
        )

    def t_copy(index, to_z, to_core, slot):
        at = text_at(index)
        return remote(
            text_out.at[at], text_out.at[at], t_send.at[slot], t_recv.at[index],
            (f, to_z * 2 + to_core),
        )

    def own_text():
        index = (z - (nz // 2 - 1)) * 2 + core
        copies = [t_copy(index, lax.rem(z + k, nz), core, k) for k in range(1, nz)]
        return copies + [t_copy(index, z, other, 0)]

    def text_step(k):
        o = jnp.where(2 * z < nz, 1 - k, k)
        owner = nz // 2 - 1 + o
        at = text_at(o * 2 + core)
        text_share[at, :] += text_sib_recv[o].astype(F32)

        def arrived(side):
            remote(
                text_send.at[0], text_recv.at[side, o], tz_send.at[0], tz_recv.at[side, o],
                (f, s),
            ).wait_recv()
            text_share[at, :] += text_recv[side, o].astype(F32)

        pl.when((z > 0) & (z <= owner))(functools.partial(arrived, 0))
        pl.when((z < nz - 1) & (z >= owner))(functools.partial(arrived, 1))
        total = text_share[at, :].astype(BF16)

        @pl.when(z != owner)
        def _():
            text_send[o] = total
            text_line(o, jnp.where(z < owner, 1, 0)).start()

        @pl.when(z == owner)
        def _():
            text_out[at, :] = total
            for copy in own_text():
                copy.start()

    def text_steps():
        swap.wait_recv()
        for k in range(2):
            text_step(k)

    def fill(k):
        zt = ordered(k)
        value = share(pl.ds(place(z, zt, 0), pair))
        low, high = value[:rows], value[rows:]
        here = core == 0
        mine[zt] = jnp.where(here, low, high)
        sib_send[zt] = jnp.where(here, high, low).astype(BF16)
        launch(
            remote(sib_send.at[zt], sib_recv.at[zt], sb_send.at[zt], sb_recv.at[zt], (f, sib))
        )

    def sib_wait(zt):
        remote(
            sib_send.at[zt], sib_recv.at[zt], sb_send.at[zt], sb_recv.at[zt], (f, s)
        ).wait_recv()

    def combined(zt, cut):
        at = pl.ds(*cut)
        return mine[zt, at, :] + sib_recv[zt, at, :].astype(F32)

    def line_copy(zt, ch, to_z):
        slot = jnp.where((to_z < z) & (zt == to_z), nz, zt)
        at = pl.ds(*cuts[ch])
        return remote(
            line_send.at[zt, at], line_recv.at[slot, at], zs_send.at[zt, ch],
            zs_recv.at[slot, ch], (f, to_z * 2 + core),
        )

    def line_wait(slot, ch):
        at = pl.ds(*cuts[ch])
        remote(
            line_send.at[0, at], line_recv.at[slot, at], zs_send.at[0, ch],
            zs_recv.at[slot, ch], (f, s),
        ).wait_recv()

    def originate(k):
        zt = ordered(k)
        sib_wait(zt)
        for ch in range(CHUNKS):
            line_send[zt, pl.ds(*cuts[ch]), :] = combined(zt, cuts[ch]).astype(BF16)
            line_copy(zt, ch, jnp.where(z == 0, 1, nz - 2)).start()

    def pass_on(zt, ch, to_z):
        at = pl.ds(*cuts[ch])
        line_wait(zt, ch)
        total = combined(zt, cuts[ch]) + line_recv[zt, at, :].astype(F32)
        line_send[zt, at, :] = total.astype(BF16)
        line_copy(zt, ch, to_z).start()

    targets = [partner] + peers + corners

    def term(k):
        target = f if k == nf - 1 else targets[k]
        value = jnp.dot(tokens_t[w_at(target), :], grads[...], preferred_element_type=F32)
        if k < nf - 1:
            w_send[k] = value.astype(BF16)
            launch(
                remote(w_send.at[k], w_recv.at[f], ws_send.at[k], ws_recv.at[f], (target, s))
            )
        else:
            rounded = value.astype(BF16).astype(F32)
            for c in range(parts):
                weight_out[c] = rounded[:, c * own_width : (c + 1) * own_width]

    fill(0)
    pl.when(ends)(text_steps)
    for k in range(1, nz):
        fill(k)
        pl.when(ends)(functools.partial(originate, k - 1))
        if k <= nf:
            term(k - 1)
    for k in range(nz - 1, nf):
        term(k)

    for k in range(1, ns):
        source = lax.rem(s - k + ns, ns)
        remote(
            gain_all.at[source], gain_all.at[source], g_send.at[k], g_recv.at[source], (f, s)
        ).wait_recv()
    gain = gain_all[0]
    for i in range(1, ns):
        gain += gain_all[i]
    gain_rows[f] = gain
    for k in range(1, nf):
        launch(
            remote(
                gain_rows.at[f], gain_rows.at[f], h_send.at[k], h_recv.at[f],
                (lax.rem(f + k, nf), s),
            )
        )

    @pl.when(middle)
    def _():
        text_steps()
        for k in range(nz):
            sib_wait(ordered(k))
        for t in range(nz - 1):
            for ch in range(CHUNKS):
                down = t - (nz - 1) + z
                pl.when(down >= 0)(functools.partial(pass_on, down, ch, z - 1))
                pl.when(t >= z)(functools.partial(pass_on, nz - 1 + z - t, ch, z + 1))

    pl.when(ends)(functools.partial(sib_wait, z))

    def finish(ch):
        at = pl.ds(*cuts[ch])

        def arrived(slot):
            line_wait(slot, ch)
            mine[z, at, :] += line_recv[slot, at, :].astype(F32)

        pl.when(down_ok)(functools.partial(arrived, z))
        pl.when(up_ok)(functools.partial(arrived, nz))
        image_out[at, :] = combined(z, cuts[ch]).astype(BF16)

    def t_wait(index):
        t_copy(index, z, core, 0).wait_recv()

    center = nz // 2 - 1
    for o in range(2):
        index = o * 2 + core

        @pl.when(z != center + o)
        def _(index=index, o=o):
            t_wait(index)
            t_copy(index, z, other, nz + o).start()

    def drain(items):
        for where, copy in items:
            if where is None:
                copy.wait_send()
            else:
                pl.when(where)(copy.wait_send)

    drain(pending[:early])
    finish(0)
    for q in targets:
        remote(
            w_send.at[0], w_recv.at[q], ws_send.at[0], ws_recv.at[q], (f, s)
        ).wait_recv()
        for c in range(parts):
            weight_out[c] += w_recv[q, :, c * own_width : (c + 1) * own_width].astype(F32)
    for k in range(1, nf):
        source = lax.rem(f - k + nf, nf)
        remote(
            gain_rows.at[source], gain_rows.at[source], h_send.at[k], h_recv.at[source], (f, s)
        ).wait_recv()
    gain = gain_rows[0]
    for i in range(1, nf):
        gain += gain_rows[i]
    gain_out[...] = gain[:2]

    for ch in range(1, CHUNKS):
        finish(ch)
    for o in range(2):
        t_wait(o * 2 + other)

    drain(pending[early:])
    for ch in range(CHUNKS):
        for k in range(nz - 1):
            pl.when(ends)(line_copy(ordered(k), ch, jnp.where(z == 0, 1, nz - 2)).wait_send)

            def sent(zt, ch=ch):
                pl.when(zt != z)(line_copy(zt, ch, z).wait_send)

        for k in range(nz):
            pl.when(middle)(functools.partial(sent, k))
    for o in range(2):
        owner = center + o
        pl.when(z != owner)(text_line(o, jnp.where(z < owner, 1, 0)).wait_send)
        pl.when(z != owner)(t_copy(o * 2 + core, z, other, nz + o).wait_send)

    @pl.when((z == center) | (z == center + 1))
    def _():
        for copy in own_text():
            copy.wait_send()


def emit(*refs):
    sems = refs[-1]
    count = len(refs) // 2
    copies = [
        pltpu.make_async_copy(refs[i], refs[count + i], sems.at[i]) for i in range(count)
    ]
    for copy in copies:
        copy.start()
    for copy in copies:
        copy.wait()


def local(nf, ns, image_input, text_input, w_qkv, query_gain, key_gain, image_up, text_up):
    _, rows, depth = image_input.shape
    text_rows = text_input.shape[1]
    w_rows, three, all_width = w_qkv.shape
    own_width = all_width // ns
    head = query_gain.shape[0]
    heads = own_width // head
    length = text_rows + rows * ns
    nz = ns // 2
    width3 = three * own_width
    piece = text_rows // 4
    block = max(b for b in range(128, 385, 128) if length % b == 0)
    vmem = pl.BlockSpec(memory_space=pltpu.VMEM)
    hbm = pl.BlockSpec(memory_space=pl.ANY)
    dma = pltpu.SemaphoreType.DMA
    results = pl.pallas_call(
        functools.partial(kernel, nf, ns),
        out_shape=(
            pltpu.VMEM((rows, depth), BF16),
            pltpu.VMEM((text_rows, depth), BF16),
            pltpu.VMEM((three, w_rows, own_width), F32),
            pltpu.VMEM((2, head), F32),
        ),
        in_specs=[hbm, hbm, hbm, hbm, hbm, vmem, vmem],
        out_specs=(vmem,) * 4,
        scratch_shapes=[
            pltpu.VMEM((length, depth), BF16),
            pltpu.VMEM((depth, width3), BF16),
            pltpu.VMEM((length, own_width), BF16),
            pltpu.VMEM((length, width3), BF16),
            pltpu.VMEM((length, width3), BF16),
            pltpu.VMEM((heads, length, head), BF16),
            pltpu.VMEM((heads, length, head), BF16),
            pltpu.VMEM((heads, head, length), BF16),
            pltpu.VMEM((heads, length, head), F32),
            pltpu.VMEM((heads, length, head), F32),
            pltpu.VMEM((length, block), F32),
            pltpu.VMEM((length, block), F32),
            pltpu.VMEM((length, block), BF16),
            pltpu.VMEM((length, block), BF16),
            pltpu.VMEM((nz, rows, depth), BF16),
            pltpu.VMEM((nz, rows, depth), BF16),
            pltpu.VMEM((nz, rows, depth), F32),
            pltpu.VMEM((nz, rows, depth), BF16),
            pltpu.VMEM((nz + 1, rows, depth), BF16),
            pltpu.VMEM((nf - 1, w_rows, width3), BF16),
            pltpu.VMEM((nf, w_rows, width3), BF16),
            pltpu.VMEM((ns, 8, head), F32),
            pltpu.VMEM((nf, 8, head), F32),
            pltpu.VMEM((text_rows, depth), F32),
            pltpu.VMEM((2, piece, depth), BF16),
            pltpu.VMEM((2, piece, depth), BF16),
            pltpu.VMEM((2, piece, depth), BF16),
            pltpu.VMEM((2, 2, piece, depth), BF16),
            pltpu.VMEM((depth, length), BF16),
            dma((3 * CHUNKS + 4 * (nz - 1) * CHUNKS,)), dma((ns, CHUNKS)),
            dma((heads, 1 + 4 * (nz - 1))), dma((heads, ns)),
            dma((2 + 4 * (nf // 2 - 1),)), dma((nf, 2)),
            dma((nz,)), dma((nz,)),
            dma((nz, CHUNKS)), dma((nz + 1, CHUNKS)),
            dma((nf,)), dma((nf,)),
            dma((ns,)), dma((ns,)),
            dma((nf,)), dma((nf,)),
            dma((nz + 2,)), dma((4,)),
            dma((1,)), dma((1,)), dma((2,)), dma((2, 2)),
            dma((4 + three,)),
        ],
        compiler_params=pltpu.CompilerParams(
            collective_id=0, has_side_effects=True, vmem_limit_bytes=56 * 1024 * 1024
        ),
        name="joint_backward",
    )(
        image_input[0], text_input[0], w_qkv.transpose(1, 0, 2), image_up[0], text_up[0],
        query_gain.reshape(1, head), key_gain.reshape(1, head),
    )
    image_grad, text_grad, weight_grad, gain = pl.pallas_call(
        emit,
        out_shape=tuple(jax.ShapeDtypeStruct(r.shape, r.dtype) for r in results),
        in_specs=[hbm] * 4,
        out_specs=(hbm,) * 4,
        scratch_shapes=[dma((4,))],
        compiler_params=pltpu.CompilerParams(vmem_limit_bytes=1024 * 1024),
        name="emit",
    )(*results)
    return (
        image_grad[None],
        text_grad[None],
        weight_grad.transpose(1, 0, 2),
        gain,
    )


def solution(mesh):
    return jax.shard_map(
        functools.partial(local, mesh.shape["fsdp"], mesh.shape["seq"]),
        mesh=mesh,
        in_specs=(
            P("fsdp", "seq", None),
            P("fsdp", None, None),
            P("fsdp", None, None),
            P(),
            P(),
            P("fsdp", "seq", None),
            P("fsdp", None, None),
        ),
        out_specs=(P("fsdp", "seq", None), P("fsdp", None, None), P("fsdp", None, "seq"), P()),
        check_vma=False,
    )
```
